32 devices in a mesh: sx: 4 (over x, core), sy: 4 (over z), dp: 2 (over y).
Axes of the slice: x: 2, y: 2, z: 4, core: 2. Of those that a mesh axis runs over, the one named last changes fastest.
Arguments:
- tokens: bfloat16 [2, 8192, 1280], P('dp', ('sx', 'sy')), may hold values from -6 to 6
- lengths: int32 [2, 64], P('dp'), may hold values from 1 to 512, 8192 in all within a row
- ln_gain: float32 [1280], replicated, may hold values from 0.1 to 1.9
- w_qkv: bfloat16 [1280, 3840], P('dp'), may hold values from -4 to 4, as said below
- w_out: bfloat16 [1280, 1280], P('dp'), may hold values from -0.15625 to 0.15625
Outputs:
- hidden: bfloat16 [2, 8192, 1280], P('dp', ('sx', 'sy'))
- pooled: float32 [2, 64, 1280], P('dp')
The draws below stay inside these ranges and needn't reach their ends.
Inputs may be any that keep to these rules, and one draw needn't show every extreme that they name: The 64 lengths of a row sum to 8192; images are packed end to end in order. `w_qkv`: columns are queries, then keys, then values, each of 16 heads of 80 columns.
All inputs are finite; a program needn't handle non-finite values.
Results may differ from the reference program's by a relative error of at most 0.0051.
Values may be sent and summed in bfloat16 or wider, within the bound.
A program may use at most 128 MiB of HBM per device.

```python
import math
import jax
import jax.numpy as jnp
import numpy as np
from jax import lax

D = 1280
HEADS = 16
MAXLEN = 512
ROWS = 2
SEQ = 8192
IMAGES = 64


def draw_w_qkv(key, part):
    first = jax.random.fold_in(jax.random.fold_in(key, 11), 0)
    base = jax.random.normal(first, (D, 3 * D), jnp.float32) * D ** (-0.5)
    return jnp.clip(base, -4.0, 4.0).astype(jnp.bfloat16)


def block_levels(rng, dims, pieces, least, largest):
    def one(position, shards_of):
        steps = jax.random.uniform(jax.random.fold_in(jax.random.fold_in(rng, 6), position), (shards_of,), jnp.float32, least / len(pieces), largest / len(pieces))
        return jnp.repeat(jnp.exp(steps), dims[position] // shards_of).reshape((-1,) + (1,) * (len(dims) - position - 1))

    loudness = one(*pieces[0])
    for cut in pieces[1:]:
        loudness = loudness * one(*cut)
    return loudness


def split_up(number_of, total, limit, lean):
    portions = [(1 << 20) // math.isqrt(standing ** lean) + 1 for standing in range(2, number_of + 1)]
    spare, given = total - limit - (number_of - 1), [1] * (number_of - 1)
    while spare > 0:
        candidates = [i for i in range(number_of - 1) if given[i] < limit]
        whole, remaining = sum([portions[i] for i in candidates]), spare
        for i in candidates:
            extra = min(limit - given[i], max(1, remaining * portions[i] // whole), spare)
            given[i] = given[i] + extra
            spare = spare - extra
    return np.array([limit] + given)


def ragged_sizes(stream_key, number_of, total, limit, lean):
    if number_of == 2:
        one = jax.random.randint(stream_key, (), max(1, total - limit), min(limit, total - 1) + 1)
        return jnp.stack([one, total - one])
    sizes = jnp.asarray(split_up(number_of, total, limit, lean), jnp.int32)
    twos = (number_of - 1) // 2
    donor, taker = sizes[1:1 + 2 * twos:2], sizes[2:2 + 2 * twos:2]
    room = jnp.minimum(donor - 1, limit - taker)
    passed = jax.random.randint(jax.random.fold_in(stream_key, 1), (twos,), 0, 1 << 20) % (room + 1)
    sizes = sizes.at[1:1 + 2 * twos:2].set(donor - passed).at[2:2 + 2 * twos:2].set(taker + passed)
    return sizes[jax.random.permutation(jax.random.fold_in(stream_key, 2), number_of)]


def gaussian(stream_key, shape, scale, bound, cuts=(), held_as=jnp.bfloat16):
    result = scale * jax.random.normal(stream_key, shape, jnp.float32)
    if cuts:
        result = result * block_levels(stream_key, shape, cuts, -0.22, 0.18)
    return jnp.clip(result, -bound, bound).astype(held_as)


def setup_inputs(seed: int = 0) -> dict:
    splits = jax.random.split(jax.random.key(seed), 6)
    tokens = gaussian(splits[0], (ROWS, SEQ, D), 1.0, 6.0, ((0, 2), (1, 16)))
    lengths = jax.vmap(lambda own: ragged_sizes(own, IMAGES, SEQ, MAXLEN, 2))(jax.random.split(splits[1], ROWS)).reshape((ROWS, IMAGES)).astype(jnp.int32)
    ln_gain = jnp.clip(1.0 + 0.18 * jax.random.normal(splits[2], (D,), jnp.float32), 0.1, 1.9)
    w_qkv = draw_w_qkv(jax.random.fold_in(splits[5], 71), 0)
    w_out = gaussian(splits[4], (D, D), D ** -0.5, 0.15625, ((0, 2),))
    return {"tokens": tokens, "lengths": lengths, "ln_gain": ln_gain, "w_qkv": w_qkv, "w_out": w_out}


def image_ids(lengths, positions, total):
    offsets = jnp.cumsum(lengths) - lengths
    counted = lax.optimization_barrier(jnp.sum((offsets[None, :] <= positions[:, None]).astype(jnp.int32), axis=1)) - 1
    inside = (positions >= 0) & (positions < total)
    return jnp.where(inside, counted, -1).astype(jnp.int32)

def normalize(rows, ln_gain):
    values = rows.astype(jnp.float32)
    center = values - lax.optimization_barrier(jnp.mean(values, axis=-1, keepdims=True))
    spread = lax.optimization_barrier(jnp.mean(center * center, axis=-1, keepdims=True))
    return (center * lax.rsqrt(spread + 1e-05) * ln_gain).astype(jnp.bfloat16)

def attend(queries, keys, values, q_ids, k_ids, margin):
    length = queries.shape[0]
    heads = queries.shape[1]
    block = min(512, length)
    window = block + 2 * margin
    scale = queries.shape[2] ** (-0.5)

    def one_block(index):
        start = (index * block).astype(jnp.int32)
        q_blk = lax.dynamic_slice_in_dim(queries, start, block, 0)
        k_blk = lax.dynamic_slice_in_dim(keys, start, window, 0)
        v_blk = lax.dynamic_slice_in_dim(values, start, window, 0)
        q_lab = lax.dynamic_slice_in_dim(q_ids, start, block, 0)
        k_lab = lax.dynamic_slice_in_dim(k_ids, start, window, 0)
        allowed = q_lab[:, None] == k_lab[None, :]

        def one_head(head):
            q_head = lax.dynamic_index_in_dim(q_blk, head, 1, keepdims=False)
            k_head = lax.dynamic_index_in_dim(k_blk, head, 1, keepdims=False)
            v_head = lax.dynamic_index_in_dim(v_blk, head, 1, keepdims=False)
            scores = jnp.dot(q_head, k_head.T, preferred_element_type=jnp.float32) * scale
            scores = jnp.where(allowed, scores, -1e+30)
            top = lax.optimization_barrier(jnp.max(scores, axis=1, keepdims=True))
            weights = jnp.exp(scores - top)
            probs = (weights / lax.optimization_barrier(jnp.sum(weights, axis=1, keepdims=True))).astype(jnp.bfloat16)
            return jnp.dot(probs, v_head, preferred_element_type=jnp.float32).astype(jnp.bfloat16)
        outcome = lax.map(one_head, jnp.arange(heads, dtype=jnp.int32))
        return jnp.transpose(outcome, (1, 0, 2))
    blocks = lax.map(one_block, jnp.arange(length // block, dtype=jnp.int32))
    return blocks.reshape(length, heads, -1)

def reference(tokens, lengths, ln_gain, w_qkv, w_out):
    total = tokens.shape[1]
    width = tokens.shape[2]
    size = width // HEADS
    positions = jnp.arange(total, dtype=jnp.int32)
    extended = jnp.arange(total + 2 * MAXLEN, dtype=jnp.int32) - MAXLEN

    def one_row(pair):
        row, lens = pair
        normed = normalize(row, ln_gain)
        qkv = jnp.dot(normed, w_qkv, preferred_element_type=jnp.float32).astype(jnp.bfloat16)
        qkv = qkv.reshape(total, 3, HEADS, size)
        own_ids = image_ids(lens, positions, total)
        far_ids = image_ids(lens, extended, total)
        padding = jnp.zeros((MAXLEN, 3, HEADS, size), jnp.bfloat16)
        padded = jnp.concatenate([padding, qkv, padding], axis=0)
        context = attend(qkv[:, 0], padded[:, 1], padded[:, 2], own_ids, far_ids, MAXLEN)
        mixed = jnp.dot(context.reshape(total, width), w_out, preferred_element_type=jnp.float32)
        hidden = (row.astype(jnp.float32) + mixed).astype(jnp.bfloat16)
        onehot = (jnp.arange(IMAGES, dtype=jnp.int32)[:, None] == own_ids[None, :]).astype(jnp.bfloat16)
        sums = jnp.dot(onehot, hidden, preferred_element_type=jnp.float32)
        pooled = sums / lens.astype(jnp.float32)[:, None]
        return (hidden, pooled)
    hidden, pooled = lax.map(one_row, (tokens, lengths))
    return (hidden, pooled)
```

```python
import functools

import jax
import jax.numpy as jnp
from jax import lax
from jax.experimental import pallas as pl
from jax.experimental.pallas import tpu as pltpu
from jax.sharding import PartitionSpec as P

HEADS = 16
MAXLEN = 512
MESH = pl.DeviceIdType.MESH
CHUNKS = 5
HALO_CHUNKS = 2
QBLOCK = 128
KBLOCK = 256
LANES = 128
FAR = -1e30


def remote(src, dst, send, recv, device):
    return pltpu.make_async_remote_copy(
        src_ref=src, dst_ref=dst, send_sem=send, recv_sem=recv, device_id=device, device_id_type=MESH
    )


def project_kernel(
    nx, ny, tok, gain, wq, wo, q_out, k_out, v_out, wo_out,
    toks, normed, wq_full, wo_full,
    y_send, y_recv, x_send, x_recv, d_send, d_recv, h_send, h_recv, local_sem,
):
    sx, sy, dp = lax.axis_index("sx"), lax.axis_index("sy"), lax.axis_index("dp")
    chips = nx // 2
    chip, core = sx // 2, lax.rem(sx, 2)
    count = nx * ny
    shard = sx * ny + sy
    before, after = lax.rem(shard + count - 1, count), lax.rem(shard + 1, count)
    prev_id = (before // ny, lax.rem(before, ny), dp)
    next_id = (after // ny, lax.rem(after, ny), dp)
    y_id = (sx, sy, 1 - dp)
    partner = (chip * 2 + 1 - core, sy, dp)

    def chip_id(step):
        return (lax.rem(chip + step, chips) * 2 + core, sy, dp)

    local, width = tok.shape
    half = wq.shape[0]
    quarter = half // nx
    piece = quarter // CHUNKS

    def rows(owner, slot, j):
        return pl.ds(pl.multiple_of(owner * half + slot * quarter + j * piece, piece), piece)

    barrier = pltpu.get_barrier_semaphore()
    greeted = [prev_id, next_id, y_id, partner] + [chip_id(s) for s in range(1, chips)]
    for device in greeted:
        pl.semaphore_signal(barrier, inc=1, device_id=device, device_id_type=MESH)
    own_tokens = pltpu.make_async_copy(tok, toks.at[pl.ds(MAXLEN, local)], local_sem.at[0])
    own_q = pltpu.make_async_copy(wq, wq_full.at[pl.ds(pl.multiple_of(dp * half, half), half)], local_sem.at[1])
    own_o = pltpu.make_async_copy(wo, wo_full.at[pl.ds(pl.multiple_of(dp * half, half), half)], local_sem.at[2])
    own_tokens.start()
    own_q.start()
    own_o.start()
    pl.semaphore_wait(barrier, len(greeted))

    weights = ((wq, wq_full), (wo, wo_full))
    hop = MAXLEN // HALO_CHUNKS
    sends = []
    for w, (part, full) in enumerate(weights):
        for j in range(CHUNKS):
            copy = remote(
                part.at[pl.ds(pl.multiple_of(sx * quarter + j * piece, piece), piece)],
                full.at[rows(dp, sx, j)], y_send.at[w, j], y_recv.at[w, j], y_id,
            )
            copy.start()
            sends.append(copy)

    def up(j):
        return remote(
            tok.at[pl.ds(local - MAXLEN + j * hop, hop)], toks.at[pl.ds(j * hop, hop)],
            h_send.at[0, j], h_recv.at[0, j], next_id,
        )

    def down(j):
        return remote(
            tok.at[pl.ds(j * hop, hop)], toks.at[pl.ds(MAXLEN + local + j * hop, hop)],
            h_send.at[1, j], h_recv.at[1, j], prev_id,
        )

    first, last = shard == 0, shard == count - 1

    @pl.when(jnp.logical_not(last))
    def _():
        for j in range(HALO_CHUNKS):
            up(j).start()

    @pl.when(jnp.logical_not(first))
    def _():
        for j in range(HALO_CHUNKS):
            down(j).start()

    @pl.when(first)
    def _():
        toks[pl.ds(0, MAXLEN)] = jnp.zeros((MAXLEN, width), toks.dtype)

    @pl.when(last)
    def _():
        toks[pl.ds(MAXLEN + local, MAXLEN)] = jnp.zeros((MAXLEN, width), toks.dtype)

    def norm(start, size):
        step = 64

        @pl.loop(0, size // step)
        def _(i):
            where = pl.ds(pl.multiple_of(start + i * step, step), step)
            values = toks[where].astype(jnp.float32)
            center = values - jnp.mean(values, axis=-1, keepdims=True)
            spread = jnp.mean(center * center, axis=-1, keepdims=True)
            normed[where] = (center * lax.rsqrt(spread + 1e-05) * gain[...]).astype(normed.dtype)

    def project(start, size, out, out_start, which):
        cols = 256

        @pl.loop(0, width // cols)
        def _(c):
            at = pl.multiple_of(c * cols, cols)
            product = jnp.dot(
                normed[pl.ds(start, size)], wq_full[:, pl.ds(which * width + at, cols)],
                preferred_element_type=jnp.float32,
            )
            out[pl.ds(out_start, size), pl.ds(at, cols)] = product.astype(out.dtype)

    own_tokens.wait()
    norm(MAXLEN, local)

    def relay(w):
        full = weights[w][1]

        def pass_across(step, j):
            slot = lax.rem(chip + chips - step, chips) * 2 + core
            here = full.at[rows(1 - dp, slot, j)]
            if step == 0:
                remote(here, here, y_send.at[w, j], y_recv.at[w, j], y_id).wait_recv()
                for s in range(1, chips):
                    copy = remote(here, here, x_send.at[w, s - 1, j], x_recv.at[w, s - 1, j], chip_id(s))
                    copy.start()
                    sends.append(copy)
            else:
                remote(here, here, x_send.at[w, step - 1, j], x_recv.at[w, step - 1, j], y_id).wait_recv()
            copy = remote(here, here, d_send.at[w, step, j], d_recv.at[w, step, j], partner)
            copy.start()
            sends.append(copy)

        for j in range(CHUNKS + 1):
            if j < CHUNKS:
                pass_across(0, j)
            if j > 0:
                for step in range(1, chips):
                    pass_across(step, j - 1)

    def finish(w):
        full = weights[w][1]
        for step in range(chips):
            slot = lax.rem(chip + chips - step, chips) * 2 + 1 - core
            for j in range(CHUNKS):
                here = full.at[rows(1 - dp, slot, j)]
                remote(here, here, d_send.at[w, step, j], d_recv.at[w, step, j], partner).wait_recv()

    relay(0)
    own_q.wait()
    finish(0)
    project(MAXLEN, local, q_out, 0, 0)
    relay(1)
    project(MAXLEN, local, k_out, MAXLEN, 1)
    project(MAXLEN, local, v_out, MAXLEN, 2)
    own_o.wait()
    finish(1)
    out_copy = pltpu.make_async_copy(wo_full, wo_out, local_sem.at[3])
    out_copy.start()
    for j in range(HALO_CHUNKS):
        for side in range(2):
            start = side * (MAXLEN + local) + j * hop

            @pl.when(jnp.logical_not(last if side else first))
            def _():
                (down if side else up)(j).wait_recv()

            norm(start, hop)
            project(start, hop, k_out, start, 1)
            project(start, hop, v_out, start, 2)

    out_copy.wait()

    @pl.when(jnp.logical_not(last))
    def _():
        for j in range(HALO_CHUNKS):
            up(j).wait_send()

    @pl.when(jnp.logical_not(first))
    def _():
        for j in range(HALO_CHUNKS):
            down(j).wait_send()

    for copy in sends:
        copy.wait_send()


def project_all(nx, ny, tok, gain, wq, wo):
    local, width = tok.shape
    long = local + 2 * MAXLEN
    bf16 = jnp.bfloat16
    chips = nx // 2
    anywhere = pl.BlockSpec(memory_space=pl.ANY)
    vmem = pl.BlockSpec(memory_space=pltpu.VMEM)
    dma = pltpu.SemaphoreType.DMA
    shape = jax.ShapeDtypeStruct
    return pl.pallas_call(
        functools.partial(project_kernel, nx, ny),
        out_shape=(
            shape((local, width), bf16), shape((long, width), bf16),
            shape((long, width), bf16), shape((width, width), bf16),
        ),
        in_specs=[anywhere, vmem, anywhere, anywhere],
        out_specs=(vmem, vmem, vmem, anywhere),
        scratch_shapes=[
            pltpu.VMEM((long, width), bf16), pltpu.VMEM((long, width), bf16),
            pltpu.VMEM((width, 3 * width), bf16), pltpu.VMEM((width, width), bf16),
            dma((2, CHUNKS)), dma((2, CHUNKS)),
            dma((2, max(chips - 1, 1), CHUNKS)), dma((2, max(chips - 1, 1), CHUNKS)),
            dma((2, chips, CHUNKS)), dma((2, chips, CHUNKS)),
            dma((2, HALO_CHUNKS)), dma((2, HALO_CHUNKS)), dma((4,)),
        ],
        compiler_params=pltpu.CompilerParams(
            collective_id=0, has_side_effects=True, vmem_limit_bytes=44 * 2**20
        ),
        name="project",
    )(tok, gain, wq, wo)


def head_window(head, size):
    low = head * size // LANES * LANES
    high = -(-(head + 1) * size // LANES) * LANES
    return low, high - low


def attend_kernel(
    lo_ref, nb_ref, begin, end, ids, scale_rows, q, k, v, tok, wo, hidden, pooled, context, top, total, acc
):
    local, width = q.shape
    size = width // HEADS
    long = k.shape[0]
    factor = size ** (-0.5) * 1.4426950408889634

    @pl.loop(0, local // QBLOCK)
    def _(block):
        here = pl.ds(pl.multiple_of(block * QBLOCK, QBLOCK), QBLOCK)
        low = lo_ref[block]
        top[...] = jnp.full(top.shape, FAR, jnp.float32)
        total[...] = jnp.zeros(total.shape, jnp.float32)
        acc[...] = jnp.zeros(acc.shape, jnp.float32)
        q_begin, q_end = begin[here], end[here]

        @pl.loop(0, nb_ref[block])
        def _(step):
            wanted = low + step * KBLOCK
            start = pl.multiple_of(jnp.minimum(wanted, long - KBLOCK), LANES)
            there = pl.ds(start, KBLOCK)
            at = start + lax.broadcasted_iota(jnp.int32, (QBLOCK, KBLOCK), 1)
            allowed = (at >= jnp.maximum(q_begin, wanted)) & (at < q_end)
            for head in range(HEADS):
                first, span = head_window(head, size)
                window = pl.ds(first, span)
                lane = first + lax.broadcasted_iota(jnp.int32, (QBLOCK, span), 1)
                inside = (lane >= head * size) & (lane < (head + 1) * size)
                q_head = jnp.where(inside, q[here, window], 0).astype(q.dtype)
                scores = lax.dot_general(
                    q_head, k[there, window], (((1,), (1,)), ((), ())),
                    preferred_element_type=jnp.float32,
                )
                scores = jnp.where(allowed, scores, FAR)
                old = top[head]
                new = jnp.maximum(old, jnp.max(scores, axis=1, keepdims=True))
                probs = jnp.exp2((scores - new) * factor)
                shrink = jnp.exp2((old - new) * factor)
                total[head] = total[head] * shrink + jnp.sum(probs, axis=1, keepdims=True)
                top[head] = new
                acc[head, :, :span] = acc[head, :, :span] * shrink + jnp.dot(
                    probs.astype(v.dtype), v[there, window], preferred_element_type=jnp.float32
                )

        for tile in range(width // LANES):
            base = tile * LANES
            lane = base + lax.broadcasted_iota(jnp.int32, (QBLOCK, LANES), 1)
            value = None
            for head in range(base // size, (base + LANES - 1) // size + 1):
                first, _ = head_window(head, size)
                one = acc[head, :, base - first : base - first + LANES] / total[head]
                value = one if value is None else jnp.where(lane >= head * size, one, value)
            context[here, base : base + LANES] = value.astype(context.dtype)

    images = pooled.shape[0]
    cols = 256
    labels = lax.broadcasted_iota(jnp.int32, (images, local), 0)
    onehot = jnp.where(labels == ids[...], 1.0, 0.0).astype(jnp.bfloat16)

    @pl.loop(0, width // cols)
    def _(c):
        at = pl.ds(pl.multiple_of(c * cols, cols), cols)
        mixed = jnp.dot(context[...], wo[:, at], preferred_element_type=jnp.float32)
        rounded = (tok[:, at].astype(jnp.float32) + mixed).astype(hidden.dtype)
        hidden[:, at] = rounded
        sums = jnp.dot(onehot, rounded, preferred_element_type=jnp.float32)
        pooled[:, at] = sums / scale_rows[...]


def attend_all(lo, nb, begin, end, ids, counts, q, k, v, tok, wo):
    local, width = tok.shape
    images = counts.shape[0]
    vmem = pl.BlockSpec(memory_space=pltpu.VMEM)
    smem = pl.BlockSpec(memory_space=pltpu.SMEM)
    return pl.pallas_call(
        attend_kernel,
        out_shape=(
            jax.ShapeDtypeStruct((local, width), jnp.bfloat16),
            jax.ShapeDtypeStruct((images, width), jnp.float32),
        ),
        in_specs=[smem, smem] + [vmem] * 9,
        out_specs=(vmem, vmem),
        scratch_shapes=[
            pltpu.VMEM((local, width), jnp.bfloat16),
            pltpu.VMEM((HEADS, QBLOCK, 1), jnp.float32),
            pltpu.VMEM((HEADS, QBLOCK, 1), jnp.float32),
            pltpu.VMEM((HEADS, QBLOCK, 2 * LANES), jnp.float32),
        ],
        compiler_params=pltpu.CompilerParams(vmem_limit_bytes=44 * 2**20),
        name="attend",
    )(lo, nb, begin, end, ids, counts, q, k, v, tok, wo)


def pool_kernel(nx, ny, parts, out, landed, reduced, send1, recv1, send2, recv2):
    sx, sy, dp = lax.axis_index("sx"), lax.axis_index("sy"), lax.axis_index("dp")
    count = nx * ny
    me = sx * ny + sy

    def device(step):
        peer = lax.rem(me + step, count)
        return peer, (peer // ny, lax.rem(peer, ny), dp)

    barrier = pltpu.get_barrier_semaphore()
    for step in range(1, count):
        pl.semaphore_signal(barrier, inc=1, device_id=device(step)[1], device_id_type=MESH)
    pl.semaphore_wait(barrier, count - 1)
    copies = []
    for step in range(1, count):
        peer, ident = device(step)
        copy = remote(
            parts.at[peer], landed.at[step - 1], send1.at[step - 1], recv1.at[step - 1], ident
        )
        copy.start()
        copies.append(copy)
    value = parts[me]
    for step in range(1, count):
        copies[step - 1].wait_recv()
        value = value + landed[step - 1]
    reduced[...] = value
    out[me] = value
    again = []
    for step in range(1, count):
        copy = remote(reduced, out.at[me], send2.at[step - 1], recv2.at[step - 1], device(step)[1])
        copy.start()
        again.append(copy)
    for step in range(1, count):
        source = lax.rem(me + count - step, count)
        remote(
            reduced, out.at[source], send2.at[step - 1], recv2.at[step - 1], device(step)[1]
        ).wait_recv()
    for copy in copies + again:
        copy.wait_send()


def pool_all(nx, ny, parts):
    count = nx * ny
    images, width = parts.shape
    each = images // count
    grouped = parts.reshape(count, each, width)
    vmem = pl.BlockSpec(memory_space=pltpu.VMEM)
    dma = pltpu.SemaphoreType.DMA
    out = pl.pallas_call(
        functools.partial(pool_kernel, nx, ny),
        out_shape=jax.ShapeDtypeStruct(grouped.shape, jnp.float32),
        in_specs=[vmem],
        out_specs=vmem,
        scratch_shapes=[
            pltpu.VMEM((count - 1, each, width), jnp.float32),
            pltpu.VMEM((each, width), jnp.float32),
            dma((count - 1,)), dma((count - 1,)), dma((count - 1,)), dma((count - 1,)),
        ],
        compiler_params=pltpu.CompilerParams(collective_id=1, has_side_effects=True),
        name="pool",
    )(grouped)
    return out.reshape(images, width)


def shards(nx, ny, tokens, lengths, ln_gain, w_qkv, w_out):
    local = tokens.shape[1]
    images = lengths.shape[1]
    tok = tokens[0]
    counts = lengths[0]
    shard = lax.axis_index("sx") * ny + lax.axis_index("sy")
    base = shard * local
    positions = base + jnp.arange(local, dtype=jnp.int32)
    ends = jnp.cumsum(counts)
    offsets = ends - counts
    reached = offsets[None, :] <= positions[:, None]
    ids = jnp.sum(reached.astype(jnp.int32), axis=1) - 1
    shift = base - MAXLEN
    begin = jnp.max(jnp.where(reached, offsets[None, :], 0), axis=1) - shift
    end = jnp.min(jnp.where(ends[None, :] > positions[:, None], ends[None, :], 2**30), axis=1) - shift
    low = begin[::QBLOCK] // LANES * LANES
    high = end[QBLOCK - 1 :: QBLOCK]
    blocks = (high - low + KBLOCK - 1) // KBLOCK
    q, k, v, wo = project_all(nx, ny, tok, ln_gain[None, :], w_qkv, w_out)
    hidden, parts = attend_all(
        low, blocks, begin[:, None], end[:, None], ids[None, :],
        counts.astype(jnp.float32)[:, None], q, k, v, tok, wo,
    )
    pooled = pool_all(nx, ny, parts)
    return (hidden[None], pooled[None])


def solution(mesh):
    in_specs = (P("dp", ("sx", "sy"), None), P("dp", None), P(), P("dp", None), P("dp", None))
    out_specs = (P("dp", ("sx", "sy"), None), P("dp", None, None))
    body = functools.partial(shards, mesh.shape["sx"], mesh.shape["sy"])
    return jax.shard_map(body, mesh=mesh, in_specs=in_specs, out_specs=out_specs, check_vma=False)
```

```python
import functools

import jax
import jax.numpy as jnp
from jax import lax
from jax.experimental import pallas as pl
from jax.experimental.pallas import tpu as pltpu
from jax.sharding import PartitionSpec as P

HEADS = 16
MAXLEN = 512
MESH = pl.DeviceIdType.MESH
CHUNKS = 5
HALO_CHUNKS = 2
QBLOCK = 256
KBLOCK = 256
LANES = 128
FAR = -1e30


def remote(src, dst, send, recv, device):
    return pltpu.make_async_remote_copy(
        src_ref=src, dst_ref=dst, send_sem=send, recv_sem=recv, device_id=device, device_id_type=MESH
    )


def project_kernel(
    nx, ny, tok, gain, wq, wo, q_out, k_out, v_out, wo_out,
    toks, normed, wq_full, wo_full,
    y_send, y_recv, x_send, x_recv, d_send, d_recv, h_send, h_recv, local_sem,
):
    sx, sy, dp = lax.axis_index("sx"), lax.axis_index("sy"), lax.axis_index("dp")
    chips = nx // 2
    chip, core = sx // 2, lax.rem(sx, 2)
    count = nx * ny
    shard = sx * ny + sy
    before, after = lax.rem(shard + count - 1, count), lax.rem(shard + 1, count)
    prev_id = (before // ny, lax.rem(before, ny), dp)
    next_id = (after // ny, lax.rem(after, ny), dp)
    y_id = (sx, sy, 1 - dp)
    partner = (chip * 2 + 1 - core, sy, dp)

    def chip_id(step):
        return (lax.rem(chip + step, chips) * 2 + core, sy, dp)

    local, width = tok.shape
    half = wq.shape[0]
    quarter = half // nx
    piece = quarter // CHUNKS

    def rows(owner, slot, j):
        return pl.ds(pl.multiple_of(owner * half + slot * quarter + j * piece, piece), piece)

    barrier = pltpu.get_barrier_semaphore()
    greeted = [prev_id, next_id, y_id, partner] + [chip_id(s) for s in range(1, chips)]
    for device in greeted:
        pl.semaphore_signal(barrier, inc=1, device_id=device, device_id_type=MESH)
    own_tokens = pltpu.make_async_copy(tok, toks.at[pl.ds(MAXLEN, local)], local_sem.at[0])
    own_q = pltpu.make_async_copy(wq, wq_full.at[pl.ds(pl.multiple_of(dp * half, half), half)], local_sem.at[1])
    own_o = pltpu.make_async_copy(wo, wo_full.at[pl.ds(pl.multiple_of(dp * half, half), half)], local_sem.at[2])
    own_tokens.start()
    own_q.start()
    own_o.start()
    pl.semaphore_wait(barrier, len(greeted))

    weights = ((wq, wq_full), (wo, wo_full))
    hop = MAXLEN // HALO_CHUNKS
    sends = []
    for w, (part, full) in enumerate(weights):
        for j in range(CHUNKS):
            copy = remote(
                part.at[pl.ds(pl.multiple_of(sx * quarter + j * piece, piece), piece)],
                full.at[rows(dp, sx, j)], y_send.at[w, j], y_recv.at[w, j], y_id,
            )
            copy.start()
            sends.append(copy)

    def up(j):
        return remote(
            tok.at[pl.ds(local - MAXLEN + j * hop, hop)], toks.at[pl.ds(j * hop, hop)],
            h_send.at[0, j], h_recv.at[0, j], next_id,
        )

    def down(j):
        return remote(
            tok.at[pl.ds(j * hop, hop)], toks.at[pl.ds(MAXLEN + local + j * hop, hop)],
            h_send.at[1, j], h_recv.at[1, j], prev_id,
        )

    first, last = shard == 0, shard == count - 1

    @pl.when(jnp.logical_not(last))
    def _():
        for j in range(HALO_CHUNKS):
            up(j).start()

    @pl.when(jnp.logical_not(first))
    def _():
        for j in range(HALO_CHUNKS):
            down(j).start()

    @pl.when(first)
    def _():
        toks[pl.ds(0, MAXLEN)] = jnp.zeros((MAXLEN, width), toks.dtype)

    @pl.when(last)
    def _():
        toks[pl.ds(MAXLEN + local, MAXLEN)] = jnp.zeros((MAXLEN, width), toks.dtype)

    def norm(start, size):
        step = 64

        @pl.loop(0, size // step)
        def _(i):
            where = pl.ds(pl.multiple_of(start + i * step, step), step)
            values = toks[where].astype(jnp.float32)
            center = values - jnp.mean(values, axis=-1, keepdims=True)
            spread = jnp.mean(center * center, axis=-1, keepdims=True)
            normed[where] = (center * lax.rsqrt(spread + 1e-05) * gain[...]).astype(normed.dtype)

    def project(start, size, out, out_start, which):
        cols = 256

        @pl.loop(0, width // cols)
        def _(c):
            at = pl.multiple_of(c * cols, cols)
            product = jnp.dot(
                normed[pl.ds(start, size)], wq_full[:, pl.ds(which * width + at, cols)],
                preferred_element_type=jnp.float32,
            )
            out[pl.ds(out_start, size), pl.ds(at, cols)] = product.astype(out.dtype)

    own_tokens.wait()
    norm(MAXLEN, local)

    def relay(w):
        full = weights[w][1]

        def pass_across(step, j):
            slot = lax.rem(chip + chips - step, chips) * 2 + core
            here = full.at[rows(1 - dp, slot, j)]
            if step == 0:
                remote(here, here, y_send.at[w, j], y_recv.at[w, j], y_id).wait_recv()
                for s in range(1, chips):
                    copy = remote(here, here, x_send.at[w, s - 1, j], x_recv.at[w, s - 1, j], chip_id(s))
                    copy.start()
                    sends.append(copy)
            else:
                remote(here, here, x_send.at[w, step - 1, j], x_recv.at[w, step - 1, j], y_id).wait_recv()
            copy = remote(here, here, d_send.at[w, step, j], d_recv.at[w, step, j], partner)
            copy.start()
            sends.append(copy)

        for j in range(CHUNKS + 1):
            if j < CHUNKS:
                pass_across(0, j)
            if j > 0:
                for step in range(1, chips):
                    pass_across(step, j - 1)

    def finish(w):
        full = weights[w][1]
        for step in range(chips):
            slot = lax.rem(chip + chips - step, chips) * 2 + 1 - core
            for j in range(CHUNKS):
                here = full.at[rows(1 - dp, slot, j)]
                remote(here, here, d_send.at[w, step, j], d_recv.at[w, step, j], partner).wait_recv()

    relay(0)
    own_q.wait()
    finish(0)
    project(MAXLEN, local, q_out, 0, 0)
    relay(1)
    project(MAXLEN, local, k_out, MAXLEN, 1)
    project(MAXLEN, local, v_out, MAXLEN, 2)
    own_o.wait()
    finish(1)
    out_copy = pltpu.make_async_copy(wo_full, wo_out, local_sem.at[3])
    out_copy.start()
    for j in range(HALO_CHUNKS):
        for side in range(2):
            start = side * (MAXLEN + local) + j * hop

            @pl.when(jnp.logical_not(last if side else first))
            def _():
                (down if side else up)(j).wait_recv()

            norm(start, hop)
            project(start, hop, k_out, start, 1)
            project(start, hop, v_out, start, 2)

    out_copy.wait()

    @pl.when(jnp.logical_not(last))
    def _():
        for j in range(HALO_CHUNKS):
            up(j).wait_send()

    @pl.when(jnp.logical_not(first))
    def _():
        for j in range(HALO_CHUNKS):
            down(j).wait_send()

    for copy in sends:
        copy.wait_send()


def project_all(nx, ny, tok, gain, wq, wo):
    local, width = tok.shape
    long = local + 2 * MAXLEN
    bf16 = jnp.bfloat16
    chips = nx // 2
    anywhere = pl.BlockSpec(memory_space=pl.ANY)
    vmem = pl.BlockSpec(memory_space=pltpu.VMEM)
    dma = pltpu.SemaphoreType.DMA
    shape = jax.ShapeDtypeStruct
    return pl.pallas_call(
        functools.partial(project_kernel, nx, ny),
        out_shape=(
            shape((local, width), bf16), shape((long, width), bf16),
            shape((long, width), bf16), shape((width, width), bf16),
        ),
        in_specs=[anywhere, vmem, anywhere, anywhere],
        out_specs=(vmem, vmem, vmem, anywhere),
        scratch_shapes=[
            pltpu.VMEM((long, width), bf16), pltpu.VMEM((long, width), bf16),
            pltpu.VMEM((width, 3 * width), bf16), pltpu.VMEM((width, width), bf16),
            dma((2, CHUNKS)), dma((2, CHUNKS)),
            dma((2, max(chips - 1, 1), CHUNKS)), dma((2, max(chips - 1, 1), CHUNKS)),
            dma((2, chips, CHUNKS)), dma((2, chips, CHUNKS)),
            dma((2, HALO_CHUNKS)), dma((2, HALO_CHUNKS)), dma((4,)),
        ],
        compiler_params=pltpu.CompilerParams(
            collective_id=0, has_side_effects=True, vmem_limit_bytes=32 * 2**20
        ),
        name="project",
    )(tok, gain, wq, wo)


def head_window(head, size):
    low = head * size // LANES * LANES
    high = -(-(head + 1) * size // LANES) * LANES
    return low, high - low


def attend_kernel(
    lo_ref, nb_ref, begin, end, ids, scale_rows, q, k, v, tok, wo, hidden, pooled,
    context, turned, flat, wide, top, total, acc,
):
    local, width = q.shape
    size = width // HEADS
    long = k.shape[0]
    factor = size ** (-0.5) * 1.4426950408889634

    @pl.loop(0, long // KBLOCK)
    def _(r):
        at = pl.multiple_of(r * KBLOCK, KBLOCK)
        turned[:, pl.ds(at, KBLOCK)] = v[pl.ds(at, KBLOCK)].T

    @pl.loop(0, local // QBLOCK)
    def _(block):
        here = pl.ds(pl.multiple_of(block * QBLOCK, QBLOCK), QBLOCK)
        low = lo_ref[block]
        top[...] = jnp.full(top.shape, FAR, jnp.float32)
        total[...] = jnp.zeros(total.shape, jnp.float32)
        acc[...] = jnp.zeros(acc.shape, jnp.float32)
        q_begin, q_end = begin[:, here], end[:, here]
        flat[...] = q[here].T
        for head in range(HEADS):
            first, span = head_window(head, size)
            row = first + lax.broadcasted_iota(jnp.int32, (span, QBLOCK), 0)
            inside = (row >= head * size) & (row < (head + 1) * size)
            wide[head, :span] = jnp.where(inside, flat[first : first + span], 0).astype(wide.dtype)

        @pl.loop(0, nb_ref[block])
        def _(step):
            wanted = low + step * KBLOCK
            start = pl.multiple_of(jnp.minimum(wanted, long - KBLOCK), LANES)
            there = pl.ds(start, KBLOCK)
            at = start + lax.broadcasted_iota(jnp.int32, (KBLOCK, QBLOCK), 0)
            allowed = (at >= jnp.maximum(q_begin, wanted)) & (at < q_end)
            for head in range(HEADS):
                first, span = head_window(head, size)
                own = pl.ds(head * size, size)
                scores = jnp.dot(
                    k[there, first : first + span], wide[head, :span],
                    preferred_element_type=jnp.float32,
                )
                scores = jnp.where(allowed, scores, FAR)
                old = top[head]
                new = jnp.maximum(old, jnp.max(scores, axis=0, keepdims=True))
                probs = jnp.exp2((scores - new) * factor)
                shrink = jnp.exp2((old - new) * factor)
                total[head] = total[head] * shrink + jnp.sum(probs, axis=0, keepdims=True)
                top[head] = new
                acc[own] = acc[own] * shrink + jnp.dot(
                    turned[own, there], probs.astype(v.dtype), preferred_element_type=jnp.float32
                )

        for head in range(HEADS):
            own = pl.ds(head * size, size)
            flat[own] = (acc[own] / total[head]).astype(flat.dtype)
        context[here] = flat[...].T

    images = pooled.shape[0]
    cols = 256
    labels = lax.broadcasted_iota(jnp.int32, (images, local), 0)
    onehot = jnp.where(labels == ids[...], 1.0, 0.0).astype(jnp.bfloat16)

    @pl.loop(0, width // cols)
    def _(c):
        at = pl.ds(pl.multiple_of(c * cols, cols), cols)
        mixed = jnp.dot(context[...], wo[:, at], preferred_element_type=jnp.float32)
        rounded = (tok[:, at].astype(jnp.float32) + mixed).astype(hidden.dtype)
        hidden[:, at] = rounded
        sums = jnp.dot(onehot, rounded, preferred_element_type=jnp.float32)
        pooled[:, at] = sums / scale_rows[...]


def attend_all(lo, nb, begin, end, ids, counts, q, k, v, tok, wo):
    local, width = tok.shape
    images = counts.shape[0]
    vmem = pl.BlockSpec(memory_space=pltpu.VMEM)
    smem = pl.BlockSpec(memory_space=pltpu.SMEM)
    return pl.pallas_call(
        attend_kernel,
        out_shape=(
            jax.ShapeDtypeStruct((local, width), jnp.bfloat16),
            jax.ShapeDtypeStruct((images, width), jnp.float32),
        ),
        in_specs=[smem, smem] + [vmem] * 9,
        out_specs=(vmem, vmem),
        scratch_shapes=[
            pltpu.VMEM((local, width), jnp.bfloat16),
            pltpu.VMEM((width, k.shape[0]), jnp.bfloat16),
            pltpu.VMEM((width, QBLOCK), jnp.bfloat16),
            pltpu.VMEM((HEADS, 2 * LANES, QBLOCK), jnp.bfloat16),
            pltpu.VMEM((HEADS, 1, QBLOCK), jnp.float32),
            pltpu.VMEM((HEADS, 1, QBLOCK), jnp.float32),
            pltpu.VMEM((width, QBLOCK), jnp.float32),
        ],
        compiler_params=pltpu.CompilerParams(vmem_limit_bytes=26 * 2**20),
        name="attend",
    )(lo, nb, begin, end, ids, counts, q, k, v, tok, wo)


def pool_kernel(nx, ny, parts, out, landed, reduced, send1, recv1, send2, recv2):
    sx, sy, dp = lax.axis_index("sx"), lax.axis_index("sy"), lax.axis_index("dp")
    count = nx * ny
    me = sx * ny + sy

    def device(step):
        peer = lax.rem(me + step, count)
        return peer, (peer // ny, lax.rem(peer, ny), dp)

    barrier = pltpu.get_barrier_semaphore()
    for step in range(1, count):
        pl.semaphore_signal(barrier, inc=1, device_id=device(step)[1], device_id_type=MESH)
    pl.semaphore_wait(barrier, count - 1)
    copies = []
    for step in range(1, count):
        peer, ident = device(step)
        copy = remote(
            parts.at[peer], landed.at[step - 1], send1.at[step - 1], recv1.at[step - 1], ident
        )
        copy.start()
        copies.append(copy)
    value = parts[me].astype(jnp.float32)
    for step in range(1, count):
        copies[step - 1].wait_recv()
        value = value + landed[step - 1].astype(jnp.float32)
    reduced[...] = value.astype(reduced.dtype)
    out[me] = value.astype(out.dtype)
    again = []
    for step in range(1, count):
        copy = remote(reduced, out.at[me], send2.at[step - 1], recv2.at[step - 1], device(step)[1])
        copy.start()
        again.append(copy)
    for step in range(1, count):
        source = lax.rem(me + count - step, count)
        remote(
            reduced, out.at[source], send2.at[step - 1], recv2.at[step - 1], device(step)[1]
        ).wait_recv()
    for copy in copies + again:
        copy.wait_send()


def pool_all(nx, ny, parts):
    count = nx * ny
    images, width = parts.shape
    each = images // count
    grouped = parts.astype(jnp.bfloat16).reshape(count, each, width)
    vmem = pl.BlockSpec(memory_space=pltpu.VMEM)
    dma = pltpu.SemaphoreType.DMA
    out = pl.pallas_call(
        functools.partial(pool_kernel, nx, ny),
        out_shape=jax.ShapeDtypeStruct(grouped.shape, grouped.dtype),
        in_specs=[vmem],
        out_specs=vmem,
        scratch_shapes=[
            pltpu.VMEM((count - 1, each, width), grouped.dtype),
            pltpu.VMEM((each, width), grouped.dtype),
            dma((count - 1,)), dma((count - 1,)), dma((count - 1,)), dma((count - 1,)),
        ],
        compiler_params=pltpu.CompilerParams(collective_id=1, has_side_effects=True),
        name="pool",
    )(grouped)
    return out.reshape(images, width).astype(jnp.float32)


def shards(nx, ny, tokens, lengths, ln_gain, w_qkv, w_out):
    local = tokens.shape[1]
    images = lengths.shape[1]
    tok = tokens[0]
    counts = lengths[0]
    shard = lax.axis_index("sx") * ny + lax.axis_index("sy")
    base = shard * local
    positions = base + jnp.arange(local, dtype=jnp.int32)
    ends = jnp.cumsum(counts)
    offsets = ends - counts
    reached = offsets[None, :] <= positions[:, None]
    ids = jnp.sum(reached.astype(jnp.int32), axis=1) - 1
    shift = base - MAXLEN
    begin = jnp.max(jnp.where(reached, offsets[None, :], 0), axis=1) - shift
    end = jnp.min(jnp.where(ends[None, :] > positions[:, None], ends[None, :], 2**30), axis=1) - shift
    low = begin[::QBLOCK] // LANES * LANES
    high = end[QBLOCK - 1 :: QBLOCK]
    blocks = (high - low + KBLOCK - 1) // KBLOCK
    q, k, v, wo = project_all(nx, ny, tok, ln_gain[None, :], w_qkv, w_out)
    hidden, parts = attend_all(
        low, blocks, begin[None, :], end[None, :], ids[None, :],
        counts.astype(jnp.float32)[:, None], q, k, v, tok, wo,
    )
    pooled = pool_all(nx, ny, parts)
    return (hidden[None], pooled[None])


def solution(mesh):
    in_specs = (P("dp", ("sx", "sy"), None), P("dp", None), P(), P("dp", None), P("dp", None))
    out_specs = (P("dp", ("sx", "sy"), None), P("dp", None, None))
    body = functools.partial(shards, mesh.shape["sx"], mesh.shape["sy"])
    return jax.shard_map(body, mesh=mesh, in_specs=in_specs, out_specs=out_specs, check_vma=False)
```
